128 devices in a mesh: rows: 4 (over z), cols: 8 (over y_hi, x), slabs: 4 (over y_lo, core).
Axes of the slice: x: 4, y: 4 (y_hi: 2, y_lo: 2; y = y_hi * 2 + y_lo), z: 4, core: 2. Of those that a mesh axis runs over, the one named last changes fastest.
Arguments:
- tracer: float32 [16, 512, 256, 128], P('rows', 'cols', 'slabs'), may hold values from 0.2 to 1.8
- crowding: float32 [16, 512, 256, 128], P('rows', 'cols', 'slabs'), may hold values from 0.5 to 2
Outputs:
- column_sum: float32 [16, 512, 256, 128], P('rows', 'cols', 'slabs')
- tracer_end: float32 [16, 512, 256, 128], P('rows', 'cols', 'slabs')
The draws below stay inside these ranges and needn't reach their ends.
All inputs are finite; a program needn't handle non-finite values.
Results may differ from the reference program's by a relative error of at most 0.00002.
Values sent between devices are 32-bit elements; how exact they have to be, the bound alone decides.
No kernel may reach another device: no remote copies, remote signals or barrier semaphores. Data moves between devices by JAX's collectives and lax.ppermute only.
A program may use at most 320 MiB of HBM per device.

```python
import jax
import jax.numpy as jnp
from jax import lax

GRID_Y = 16
GRID_X = 512
GRID_Z = 256
LEVELS = 128
STEPS = 4


def shard_levels(own_key, shape, cuts, low, top_value):
    def one(dim, shards_of):
        steps = jax.random.uniform(jax.random.fold_in(jax.random.fold_in(own_key, 6), dim), (shards_of,), jnp.float32, low / len(cuts), top_value / len(cuts))
        return jnp.repeat(jnp.exp(steps), shape[dim] // shards_of).reshape((-1,) + (1,) * (len(shape) - dim - 1))

    factor_of = one(*cuts[0])
    for cut in cuts[1:]:
        factor_of = factor_of * one(*cut)
    return factor_of


def setup_inputs(seed: int = 0) -> dict:
    splits = jax.random.split(jax.random.key(seed), 3)
    tracer = jnp.clip(0.2 + 1.5999999 * jax.random.uniform(splits[0], (GRID_Y, GRID_X, GRID_Z, LEVELS), jnp.float32) ** shard_levels(splits[0], (GRID_Y, GRID_X, GRID_Z, LEVELS), ((0, 4), (1, 8), (2, 4)), -0.2, 0.2), 0.2, 1.8)
    crowding = jnp.clip(0.5 + 1.5 * jax.random.uniform(splits[1], (GRID_Y, GRID_X, GRID_Z, LEVELS), jnp.float32) ** shard_levels(splits[1], (GRID_Y, GRID_X, GRID_Z, LEVELS), ((0, 4), (1, 8), (2, 4)), -0.2, 0.2), 0.5, 2.0)
    return {"tracer": tracer, "crowding": crowding}


def inner_cells(values, dims):
    for dim in dims:
        values = lax.slice_in_dim(values, 1, values.shape[dim] - 1, axis=dim)
    return values


def side_cells(values, dim, start, dims):
    others = [other for other in dims if other != dim]
    values = inner_cells(values, others)
    return lax.slice_in_dim(values, start, start + values.shape[dim] - 2, axis=dim)


def advance(padded, crowding):
    middle = inner_cells(padded, (0, 1, 2))
    lower = [side_cells(padded, dim, 0, (0, 1, 2)) for dim in (0, 1, 2)]
    upper = [side_cells(padded, dim, 2, (0, 1, 2)) for dim in (0, 1, 2)]
    spread = lower[0] + upper[0] + lower[1] + upper[1] + lower[2] + upper[2] - 6.0 * middle
    return middle + 0.1 * spread + 0.2 * middle * (1.0 - middle * crowding)


def reference(tracer, crowding):
    for step in range(STEPS):
        tracer = advance(jnp.pad(tracer, ((1, 1), (1, 1), (1, 1), (0, 0)), mode="constant"), crowding)
    column_sum = jnp.cumsum(tracer, axis=0) / GRID_Y
    return column_sum, tracer
```

```python
import functools

import jax
import jax.numpy as jnp
from jax import lax
from jax.experimental import pallas as pl
from jax.experimental.pallas import tpu as pltpu
from jax.sharding import PartitionSpec as P

STEPS = 4
CHUNKS = 2
PLANES = 4


def stencil(refs, chunk_x, base, masked_low):
    c, k, ylo, yhi, xlo, xhi, zlo, zhi = refs
    rows, _, zs, lanes = k.shape
    z = lax.broadcasted_iota(jnp.int32, (zs, lanes), 0)

    def plane(y, xx):
        x = base + xx
        mid = c[y, x]
        if xx == 0:
            left = jnp.where(x == 0, xlo[y, 0], c[y, jnp.maximum(x - 1, 0)])
        else:
            left = c[y, x - 1]
        if xx == k.shape[1] - 1:
            right = jnp.where(x == chunk_x - 1, xhi[y, 0], c[y, jnp.minimum(x + 1, chunk_x - 1)])
        else:
            right = c[y, x + 1]
        down = jnp.where(z == 0, zlo[y, xx], pltpu.roll(mid, 1, 0))
        up = jnp.where(z == zs - 1, zhi[y, xx], pltpu.roll(mid, zs - 1, 0))
        if y > 0:
            before = c[y - 1, x]
        elif ylo is None:
            before = masked_low * mid
        else:
            before = ylo[xx]
        if y < rows - 1:
            after = c[y + 1, x]
        elif yhi is None:
            after = mid
        else:
            after = yhi[xx]
        around = ((before + after) + (left + right)) + (down + up)
        return mid * (0.6 - (0.2 * mid) * k[y, xx]) + 0.1 * around

    return plane


def step_kernel(c, k, ylo, yhi, xlo, xhi, zlo, zhi, out, row_lo, row_hi, zlo_out, zhi_out, edge, *, chunk_x, edge_x):
    i = pl.program_id(0)
    rows, planes, zs, _ = k.shape
    plane = stencil((c, k, ylo, yhi, xlo, xhi, zlo, zhi), chunk_x, i * planes, None)
    for xx in range(planes):
        for y in range(rows):
            new = plane(y, xx)
            out[y, xx] = new
            zlo_out[y, xx] = new[0:1]
            zhi_out[y, xx] = new[zs - 1 : zs]
            if y == 0:
                row_lo[xx] = new
            if y == rows - 1:
                row_hi[xx] = new
            if edge_x is not None and edge_x % planes == xx:

                @pl.when(i == edge_x // planes)
                def _():
                    edge[y, 0] = new


def total_kernel(place, c, k, xlo, xhi, zlo, zhi, total, *, chunk_x):
    i = pl.program_id(0)
    rows, planes, _, _ = k.shape
    inside = jnp.where(place[0] > 0, 1.0, 0.0).astype(jnp.float32)
    plane = stencil((c, k, None, None, xlo, xhi, zlo, zhi), chunk_x, i * planes, inside)
    for xx in range(planes):
        value = plane(0, xx)
        for y in range(1, rows):
            value = value + plane(y, xx)
        total[xx] = value


def last_kernel(place, c, k, ylo, yhi, xlo, xhi, zlo, zhi, *rest, chunk_x):
    out, sums = rest[-2:]
    i = pl.program_id(0)
    rows, planes, _, _ = k.shape
    inside = jnp.where(place[0] > 0, 0.1, 0.0).astype(jnp.float32)
    plane = stencil((c, k, ylo, yhi, xlo, xhi, zlo, zhi), chunk_x, i * planes, None)
    for xx in range(planes):
        sofar = inside * c[0, i * planes + xx] - 0.1 * ylo[xx]
        for y in range(rows):
            new = plane(y, xx)
            out[y, xx] = new
            sofar = sofar + new
            sums[y, xx] = sofar


def add_kernel(place, sums, one, two, three, *rest, scale):
    out = rest[-1]
    rows, planes, _, _ = sums.shape
    inside = jnp.where(place[0] > 0, 1.0, 0.0).astype(jnp.float32)
    for xx in range(planes):
        below = one[xx] + inside * two[xx] + three[xx]
        for y in range(rows):
            out[y, xx] = (sums[y, xx] + below) * scale


class Source:
    def __init__(self, array, start, length):
        self.array, self.start, self.length = array, start, length

    def whole(self):
        rows, _, zs, lanes = self.array.shape
        at = self.start // self.length
        return pl.BlockSpec((rows, self.length, zs, lanes), lambda i: (0, at, 0, 0))

    def stepped(self, planes):
        rows, _, zs, lanes = self.array.shape
        at = self.start // planes
        return pl.BlockSpec((rows, planes, zs, lanes), lambda i: (0, at + i, 0, 0))

    def plane(self, x):
        rows, _, zs, lanes = self.array.shape
        at = self.start + x
        return pl.BlockSpec((rows, 1, zs, lanes), lambda i: (0, at, 0, 0))


def rows_spec(planes, zs, lanes):
    return pl.BlockSpec((planes, zs, lanes), lambda i: (i, 0, 0))


def edge_spec(rows, planes, lanes):
    return pl.BlockSpec((rows, planes, 1, lanes), lambda i: (0, i, 0, 0))


def cost(cells, per_cell):
    return pl.CostEstimate(flops=cells * per_cell, bytes_accessed=cells * 12, transcendentals=0)


SMEM = pl.BlockSpec(memory_space=pltpu.SMEM)
ANY = pl.BlockSpec(memory_space=pl.ANY)


def shifts(axis):
    count = lax.axis_size(axis)
    up = [(i, i + 1) for i in range(count - 1)]
    return up, [(b, a) for a, b in up]


def body(tracer, crowding):
    rows, xs, zs, lanes = tracer.shape
    n = CHUNKS
    size = xs // n
    planes = PLANES
    grid = (size // planes,)
    cells = rows * size * zs * lanes
    f32 = jnp.float32
    place = lax.axis_index("rows").astype(jnp.int32).reshape(1)
    row_up, row_down = shifts("rows")
    col_up, col_down = shifts("cols")
    slab_up, slab_down = shifts("slabs")
    params = pltpu.CompilerParams(dimension_semantics=("arbitrary",), vmem_limit_bytes=40 * 2**20)
    row_block = rows_spec(planes, zs, lanes)
    edge_block = edge_spec(rows, planes, lanes)
    row_shape = jax.ShapeDtypeStruct((size, zs, lanes), f32)
    edge_shape = jax.ShapeDtypeStruct((rows, size, 1, lanes), f32)

    field = [Source(tracer, j * size, size) for j in range(n)]
    crowd = [Source(crowding, j * size, size) for j in range(n)]

    def exchange_rows(lo, hi):
        return (lax.ppermute(hi, "rows", row_up), lax.ppermute(lo, "rows", row_down))

    def exchange_z(lo, hi):
        return (lax.ppermute(hi, "slabs", slab_up), lax.ppermute(lo, "slabs", slab_down))

    halo_y = [
        exchange_rows(tracer[0, j * size : (j + 1) * size], tracer[rows - 1, j * size : (j + 1) * size]) for j in range(n)
    ]
    halo_x = (lax.ppermute(tracer[:, xs - 1 : xs], "cols", col_up), lax.ppermute(tracer[:, 0:1], "cols", col_down))
    zlo_all, zhi_all = tracer[:, :, 0:1], tracer[:, :, zs - 1 : zs]
    z_all = exchange_z(zlo_all, zhi_all)
    halo_z = [(z_all[0][:, j * size : (j + 1) * size], z_all[1][:, j * size : (j + 1) * size]) for j in range(n)]

    def x_sides(field, halo_x, j):
        low = (halo_x[0], pl.BlockSpec((rows, 1, zs, lanes), lambda i: (0, 0, 0, 0))) if j == 0 else (field[j - 1].array, field[j - 1].plane(size - 1))
        high = (
            (halo_x[1], pl.BlockSpec((rows, 1, zs, lanes), lambda i: (0, 0, 0, 0)))
            if j == n - 1
            else (field[j + 1].array, field[j + 1].plane(0))
        )
        return low, high

    for step in range(STEPS - 1):
        made, next_y, next_z, edges = [], [], [], {}
        for j in range(n):
            low, high = x_sides(field, halo_x, j)
            edge_x = {0: 0, n - 1: size - 1}.get(j)
            out, lo, hi, zlo, zhi, edge = pl.pallas_call(
                functools.partial(step_kernel, chunk_x=size, edge_x=edge_x),
                grid=grid,
                in_specs=[field[j].whole(), crowd[j].stepped(planes), row_block, row_block, low[1], high[1], edge_block, edge_block],
                out_specs=[
                    pl.BlockSpec((rows, planes, zs, lanes), lambda i: (0, i, 0, 0)),
                    row_block,
                    row_block,
                    edge_block,
                    edge_block,
                    pl.BlockSpec((rows, 1, zs, lanes), lambda i: (0, 0, 0, 0)),
                ],
                out_shape=[
                    jax.ShapeDtypeStruct((rows, size, zs, lanes), f32),
                    row_shape,
                    row_shape,
                    edge_shape,
                    edge_shape,
                    jax.ShapeDtypeStruct((rows, 1, zs, lanes), f32),
                ],
                compiler_params=params,
                cost_estimate=cost(cells, 14),
                name=f"step{step}_{j}",
            )(field[j].array, crowd[j].array, *halo_y[j], low[0], high[0], *halo_z[j])
            made.append(Source(out, 0, size))
            next_y.append(exchange_rows(lo, hi))
            next_z.append(exchange_z(zlo, zhi))
            edges[j] = edge
        halo_x = (lax.ppermute(edges[n - 1], "cols", col_up), lax.ppermute(edges[0], "cols", col_down))
        field, halo_y, halo_z = made, next_y, next_z

    one, two, three = [], [], []
    for j in range(n):
        low, high = x_sides(field, halo_x, j)
        total = pl.pallas_call(
            functools.partial(total_kernel, chunk_x=size),
            grid=grid,
            in_specs=[SMEM, field[j].whole(), crowd[j].stepped(planes), low[1], high[1], edge_block, edge_block],
            out_specs=row_block,
            out_shape=row_shape,
            compiler_params=params,
            cost_estimate=cost(cells, 14),
            name=f"total_{j}",
        )(place, field[j].array, crowd[j].array, low[0], high[0], *halo_z[j])
        two.append(lax.ppermute(total, "rows", [(0, 3), (1, 0)]))
        one.append(lax.ppermute(total, "rows", row_up))
        three.append(lax.ppermute(two[j], "rows", [(3, 2), (0, 3)]))

    full = jax.ShapeDtypeStruct(tracer.shape, f32)
    end = None
    sums = []
    for j in range(n):
        low, high = x_sides(field, halo_x, j)
        operands = [place, field[j].array, crowd[j].array, *halo_y[j], low[0], high[0], *halo_z[j]]
        specs = [SMEM, field[j].whole(), crowd[j].stepped(planes), row_block, row_block, low[1], high[1], edge_block, edge_block]
        alias = {}
        if end is not None:
            alias = {len(operands): 0}
            operands.append(end)
            specs.append(ANY)
        end, partial = pl.pallas_call(
            functools.partial(last_kernel, chunk_x=size),
            grid=grid,
            in_specs=specs,
            out_specs=[
                pl.BlockSpec((rows, planes, zs, lanes), lambda i, j=j: (0, j * grid[0] + i, 0, 0)),
                pl.BlockSpec((rows, planes, zs, lanes), lambda i: (0, i, 0, 0)),
            ],
            out_shape=[full, jax.ShapeDtypeStruct((rows, size, zs, lanes), f32)],
            input_output_aliases=alias,
            compiler_params=params,
            cost_estimate=cost(cells, 18),
            name=f"last_{j}",
        )(*operands)
        sums.append(partial)

    column = None
    for j in range(n):
        operands = [place, sums[j], one[j], two[j], three[j]]
        block = pl.BlockSpec((rows, planes, zs, lanes), lambda i: (0, i, 0, 0))
        specs = [SMEM, block, row_block, row_block, row_block]
        alias = {}
        if column is not None:
            alias = {len(operands): 0}
            operands.append(column)
            specs.append(ANY)
        column = pl.pallas_call(
            functools.partial(add_kernel, scale=1.0 / (rows * lax.axis_size("rows"))),
            grid=grid,
            in_specs=specs,
            out_specs=pl.BlockSpec((rows, planes, zs, lanes), lambda i, j=j: (0, j * grid[0] + i, 0, 0)),
            out_shape=full,
            input_output_aliases=alias,
            compiler_params=params,
            cost_estimate=cost(cells, 3),
            name=f"add_{j}",
        )(*operands)
    return column, end


def solution(mesh):
    spec = P("rows", "cols", "slabs", None)
    return jax.shard_map(body, mesh=mesh, in_specs=(spec, spec), out_specs=(spec, spec), check_vma=False)
```

```python
import functools

import jax
import jax.numpy as jnp
from jax import lax
from jax.experimental import pallas as pl
from jax.experimental.pallas import tpu as pltpu
from jax.sharding import PartitionSpec as P


STEPS = 4
CHUNKS = 2
PLANES = 4
VMEM = 16 * 2**20


def stencil(refs, masked_low):
    c, before_x, after_x, k, ylo, yhi, xlo, xhi, zlo, zhi = refs
    rows, planes, zs, lanes = k.shape
    z = lax.broadcasted_iota(jnp.int32, (zs, lanes), 0)
    i, last = pl.program_id(0), pl.num_programs(0) - 1

    def plane(y, xx):
        mid = c[y, xx]
        left = c[y, xx - 1] if xx else jnp.where(i == 0, xlo[y, 0], before_x[y, 0])
        right = c[y, xx + 1] if xx < planes - 1 else jnp.where(i == last, xhi[y, 0], after_x[y, 0])
        down = jnp.where(z == 0, zlo[y, xx], pltpu.roll(mid, 1, 0))
        up = jnp.where(z == zs - 1, zhi[y, xx], pltpu.roll(mid, zs - 1, 0))
        if y > 0:
            before = c[y - 1, xx]
        elif ylo is None:
            before = masked_low * mid
        else:
            before = ylo[xx]
        if y < rows - 1:
            after = c[y + 1, xx]
        elif yhi is None:
            after = mid
        else:
            after = yhi[xx]
        around = ((before + after) + (left + right)) + (down + up)
        return mid * (0.6 - (0.2 * mid) * k[y, xx]) + 0.1 * around

    return plane


def step_kernel(c, cl, cr, k, ylo, yhi, xlo, xhi, zlo, zhi, out, row_lo, row_hi, zlo_out, zhi_out, edge, *, edge_x):
    i = pl.program_id(0)
    rows, planes, zs, _ = k.shape
    plane = stencil((c, cl, cr, k, ylo, yhi, xlo, xhi, zlo, zhi), None)
    for xx in range(planes):
        for y in range(rows):
            new = plane(y, xx)
            out[y, xx] = new
            zlo_out[y, xx] = new[0:1]
            zhi_out[y, xx] = new[zs - 1 : zs]
            if y == 0:
                row_lo[xx] = new
            if y == rows - 1:
                row_hi[xx] = new
            if edge_x is not None and edge_x % planes == xx:

                @pl.when(i == edge_x // planes)
                def _():
                    edge[y, 0] = new


def total_kernel(place, c, cl, cr, k, xlo, xhi, zlo, zhi, total):
    rows, planes, _, _ = k.shape
    inside = jnp.where(place[0] > 0, 1.0, 0.0).astype(jnp.float32)
    plane = stencil((c, cl, cr, k, None, None, xlo, xhi, zlo, zhi), inside)
    for xx in range(planes):
        value = plane(0, xx)
        for y in range(1, rows):
            value = value + plane(y, xx)
        total[xx] = value


def last_kernel(place, c, cl, cr, k, ylo, yhi, xlo, xhi, zlo, zhi, *rest):
    out, sums = rest[-2:]
    rows, planes, _, _ = k.shape
    inside = jnp.where(place[0] > 0, 0.1, 0.0).astype(jnp.float32)
    plane = stencil((c, cl, cr, k, ylo, yhi, xlo, xhi, zlo, zhi), None)
    for xx in range(planes):
        sofar = inside * c[0, xx] - 0.1 * ylo[xx]
        for y in range(rows):
            new = plane(y, xx)
            out[y, xx] = new
            sofar = sofar + new
            sums[y, xx] = sofar


def add_kernel(place, sums, one, two, three, *rest, scale):
    out = rest[-1]
    rows, planes, _, _ = sums.shape
    inside = jnp.where(place[0] > 0, 1.0, 0.0).astype(jnp.float32)
    for xx in range(planes):
        below = one[xx] + inside * two[xx] + three[xx]
        for y in range(rows):
            out[y, xx] = (sums[y, xx] + below) * scale


def in_hbm(array):
    return pltpu.with_memory_space_constraint(array, pltpu.HBM)


class Source:
    def __init__(self, array, start, length):
        self.array, self.start, self.length = in_hbm(array), start, length

    def plane(self, x):
        rows, _, zs, lanes = self.array.shape
        at = self.start + x
        return (self.array, pl.BlockSpec((rows, 1, zs, lanes), lambda i: (0, at, 0, 0)))

    def blocks(self, planes):
        rows, _, zs, lanes = self.array.shape
        at = self.start // planes
        return (self.array, pl.BlockSpec((rows, planes, zs, lanes), lambda i: (0, at + i, 0, 0)))

    def with_sides(self, planes):
        rows, _, zs, lanes = self.array.shape
        start, end = self.start, self.start + self.length - 1
        before = pl.BlockSpec((rows, 1, zs, lanes), lambda i: (0, jnp.maximum(start + i * planes - 1, start), 0, 0))
        after = pl.BlockSpec((rows, 1, zs, lanes), lambda i: (0, jnp.minimum(start + (i + 1) * planes, end), 0, 0))
        return [self.blocks(planes), (self.array, before), (self.array, after)]


def rows_spec(planes, zs, lanes):
    return pl.BlockSpec((planes, zs, lanes), lambda i: (i, 0, 0))


def edge_spec(rows, planes, lanes):
    return pl.BlockSpec((rows, planes, 1, lanes), lambda i: (0, i, 0, 0))


def cost(cells, per_cell):
    return pl.CostEstimate(flops=cells * per_cell, bytes_accessed=cells * 12, transcendentals=0)


SMEM = pl.BlockSpec(memory_space=pltpu.SMEM)
ANY = pl.BlockSpec(memory_space=pl.ANY)


def shifts(axis):
    count = lax.axis_size(axis)
    up = [(i, i + 1) for i in range(count - 1)]
    return up, [(b, a) for a, b in up]


def program(tracer, crowding):
    rows, xs, zs, lanes = tracer.shape
    n = CHUNKS
    size = xs // n
    planes = PLANES
    grid = (size // planes,)
    cells = rows * size * zs * lanes
    f32 = jnp.float32
    place = lax.axis_index("rows").astype(jnp.int32)
    row_up, row_down = shifts("rows")
    col_up, col_down = shifts("cols")
    slab_up, slab_down = shifts("slabs")
    params = pltpu.CompilerParams(dimension_semantics=("arbitrary",), vmem_limit_bytes=VMEM)
    row_block = rows_spec(planes, zs, lanes)
    edge_block = edge_spec(rows, planes, lanes)
    block = pl.BlockSpec((rows, planes, zs, lanes), lambda i: (0, i, 0, 0))
    side_block = pl.BlockSpec((rows, 1, zs, lanes), lambda i: (0, 0, 0, 0))
    row_shape = jax.ShapeDtypeStruct((size, zs, lanes), f32)
    edge_shape = jax.ShapeDtypeStruct((rows, size, 1, lanes), f32)
    full = pltpu.HBM(tracer.shape, f32)

    def call(kernel, inputs, out_specs, out_shape, per_cell, alias=None):
        extra, aliases = [], {}
        if alias is not None:
            extra, aliases = [(alias, ANY)], {len(inputs): 0}
        arrays, specs = zip(*inputs, *extra)
        return pl.pallas_call(
            kernel,
            grid=grid,
            in_specs=list(specs),
            out_specs=out_specs,
            out_shape=out_shape,
            input_output_aliases=aliases,
            compiler_params=params,
            cost_estimate=cost(cells, per_cell),
        )(*arrays)

    def send_rows(lo, hi):
        return (lax.ppermute(hi, "rows", row_up), lax.ppermute(lo, "rows", row_down))

    def send_z(lo, hi):
        return (lax.ppermute(hi, "slabs", slab_up), lax.ppermute(lo, "slabs", slab_down))

    here = (place.reshape(1), SMEM)
    field = [Source(tracer, j * size, size) for j in range(n)]
    crowd = [Source(crowding, j * size, size) for j in range(n)]

    halo_y = []
    source = tracer
    for j in range(n):
        lo, hi = (source[r, j * size : (j + 1) * size] for r in (0, rows - 1))
        lo, hi, source = lax.optimization_barrier((lo, hi, source))
        halo_y.append(send_rows(lo, hi))
    halo_x = (lax.ppermute(tracer[:, xs - 1 : xs], "cols", col_up), lax.ppermute(tracer[:, 0:1], "cols", col_down))
    z_all = send_z(tracer[:, :, 0:1], tracer[:, :, zs - 1 : zs])
    halo_z = [tuple(side[:, j * size : (j + 1) * size] for side in z_all) for j in range(n)]

    def sides(j):
        low = field[j - 1].plane(size - 1) if j else (halo_x[0], side_block)
        high = field[j + 1].plane(0) if j < n - 1 else (halo_x[1], side_block)
        return [low, high, *((side, edge_block) for side in halo_z[j])]

    def near(j):
        return [*field[j].with_sides(planes), crowd[j].blocks(planes)]

    for _ in range(STEPS - 1):
        made, next_y, next_z, edges = [], [], [], {}
        for j in range(n):
            edge_x = {0: 0, n - 1: size - 1}.get(j)
            out, lo, hi, zlo, zhi, edge = call(
                functools.partial(step_kernel, edge_x=edge_x),
                [*near(j), *((side, row_block) for side in halo_y[j]), *sides(j)],
                [block, row_block, row_block, edge_block, edge_block, side_block],
                [
                    pltpu.HBM((rows, size, zs, lanes), f32),
                    row_shape,
                    row_shape,
                    edge_shape,
                    edge_shape,
                    jax.ShapeDtypeStruct((rows, 1, zs, lanes), f32),
                ],
                14,
            )
            made.append(Source(out, 0, size))
            next_y.append(send_rows(lo, hi))
            next_z.append(send_z(zlo, zhi))
            edges[j] = edge
        halo_x = (lax.ppermute(edges[n - 1], "cols", col_up), lax.ppermute(edges[0], "cols", col_down))
        field, halo_y, halo_z = made, next_y, next_z

    total = [call(total_kernel, [here, *near(j), *sides(j)], row_block, row_shape, 14) for j in range(n)]
    one, two, three = [None] * n, [None] * n, [None] * n
    two[1] = lax.ppermute(total[1], "rows", [(0, 3), (1, 0)])
    one[0] = lax.ppermute(total[0], "rows", [(0, 1), (1, 2)])
    two[0] = lax.ppermute(total[0], "rows", [(0, 3)])
    passed = jnp.where(place == 2, total[0] + one[0], two[0])
    three[0] = lax.ppermute(passed, "rows", [(2, 3), (3, 2)])
    one[1] = lax.ppermute(total[1], "rows", row_up)
    three[1] = lax.ppermute(two[1], "rows", [(3, 2), (0, 3)])

    end, column = None, None
    sums = []
    for j in range(n):
        end, partial = call(
            last_kernel,
            [here, *near(j), *((side, row_block) for side in halo_y[j]), *sides(j)],
            [pl.BlockSpec((rows, planes, zs, lanes), lambda i, j=j: (0, j * grid[0] + i, 0, 0)), block],
            [full, pltpu.HBM((rows, size, zs, lanes), f32)],
            18,
            alias=end,
        )
        sums.append(partial)
    for j in range(n):
        column = call(
            functools.partial(add_kernel, scale=1.0 / (rows * lax.axis_size("rows"))),
            [here, (in_hbm(sums[j]), block), (one[j], row_block), (two[j], row_block), (three[j], row_block)],
            pl.BlockSpec((rows, planes, zs, lanes), lambda i, j=j: (0, j * grid[0] + i, 0, 0)),
            full,
            3,
            alias=column,
        )
    return column, end


def solution(mesh):
    spec = P("rows", "cols", "slabs", None)
    return jax.shard_map(program, mesh=mesh, in_specs=(spec, spec), out_specs=(spec, spec), check_vma=False)
```

```python
import functools
from typing import NamedTuple

import jax
import jax.numpy as jnp
from jax import lax
from jax.experimental import pallas as pl
from jax.experimental.pallas import tpu as pltpu
from jax.sharding import PartitionSpec as P


STEPS = 4
CHUNKS = 2
PLANES = 4
LIMIT = 8 * 2**20

VMEM = pl.BlockSpec(memory_space=pltpu.VMEM)
SMEM = pl.BlockSpec(memory_space=pltpu.SMEM)
ANY = pl.BlockSpec(memory_space=pl.ANY)


class At(NamedTuple):
    c: int
    k: int
    xlo: int
    xhi: int


def blocks(size, make, done=None):
    def block(i, carry):
        for xx in range(PLANES):
            make(i * PLANES + xx, xx == 0, xx == PLANES - 1)
        if done is not None:
            done(i)
        return carry

    lax.fori_loop(0, size // PLANES, block, 0)


def stencil(c, k, ylo, yhi, xlo, xhi, zlo, zhi, at, size, masked_low):
    rows, _, zs, lanes = c.shape
    z = lax.broadcasted_iota(jnp.int32, (zs, lanes), 0)

    def plane(y, x, first, last):
        mid = c[y, at.c + x]
        if first:
            left = jnp.where(x == 0, xlo[y, at.xlo], c[y, at.c + jnp.maximum(x - 1, 0)])
        else:
            left = c[y, at.c + x - 1]
        if last:
            right = jnp.where(x == size - 1, xhi[y, at.xhi], c[y, at.c + jnp.minimum(x + 1, size - 1)])
        else:
            right = c[y, at.c + x + 1]
        down = jnp.where(z == 0, zlo[y, at.k + x], pltpu.roll(mid, 1, 0))
        up = jnp.where(z == zs - 1, zhi[y, at.k + x], pltpu.roll(mid, zs - 1, 0))
        if y > 0:
            before = c[y - 1, at.c + x]
        elif ylo is None:
            before = masked_low * mid
        else:
            before = ylo[x]
        if y < rows - 1:
            after = c[y + 1, at.c + x]
        elif yhi is None:
            after = mid
        else:
            after = yhi[x]
        around = ((before + after) + (left + right)) + (down + up)
        return mid * (0.6 - (0.2 * mid) * k[y, at.k + x]) + 0.1 * around

    return plane


def step_kernel(place, c, k, ylo, yhi, xlo, xhi, zlo, zhi, *rest, at, edge_x):
    out, row_lo, row_hi, zlo_out, zhi_out, edge = rest[-6:]
    size = out.shape[1]
    rows, _, zs, _ = c.shape
    plane = stencil(c, k, ylo, yhi, xlo, xhi, zlo, zhi, at, size, None)

    def make(x, first, last):
        for y in range(rows):
            new = plane(y, x, first, last)
            out[y, x] = new
            zlo_out[y, at.k + x] = new[0:1]
            zhi_out[y, at.k + x] = new[zs - 1 : zs]
            if y == 0:
                row_lo[x] = new
            if y == rows - 1:
                row_hi[x] = new

    blocks(size, make)
    for y in range(rows):
        edge[y, 0] = out[y, edge_x]


def total_kernel(place, c, k, xlo, xhi, zlo, zhi, total, *, at):
    size = total.shape[0]
    inside = jnp.where(place[0] > 0, 1.0, 0.0).astype(jnp.float32)
    plane = stencil(c, k, None, None, xlo, xhi, zlo, zhi, at, size, inside)

    def make(x, first, last):
        value = plane(0, x, first, last)
        for y in range(1, c.shape[0]):
            value = value + plane(y, x, first, last)
        total[x] = value

    blocks(size, make)


def copies(held, out, sems, at):
    def copy(i):
        there = pl.ds(at.k + i * PLANES, PLANES)
        return pltpu.make_async_copy(held.at[:, pl.ds(i * PLANES, PLANES)], out.at[:, there], sems.at[i])

    return copy


def finish(copy, size):
    def wait(i, carry):
        copy(i).wait()
        return carry

    lax.fori_loop(0, size // PLANES, wait, 0)


def last_kernel(place, c, k, ylo, yhi, xlo, xhi, zlo, zhi, *rest, at):
    out, sums, held, sems = rest[-4:]
    size = sums.shape[1]
    inside = jnp.where(place[0] > 0, 0.1, 0.0).astype(jnp.float32)
    plane = stencil(c, k, ylo, yhi, xlo, xhi, zlo, zhi, at, size, None)
    copy = copies(held, out, sems, at)

    def make(x, first, last):
        sofar = inside * c[0, at.c + x] - 0.1 * ylo[x]
        for y in range(c.shape[0]):
            new = plane(y, x, first, last)
            held[y, x] = new
            sofar = sofar + new
            sums[y, x] = sofar

    blocks(size, make, lambda i: copy(i).start())
    finish(copy, size)


def add_kernel(place, sums, one, two, three, *rest, at, scale):
    out, held, sems = rest[-3:]
    rows, size, _, _ = sums.shape
    inside = jnp.where(place[0] > 0, 1.0, 0.0).astype(jnp.float32)
    copy = copies(held, out, sems, at)

    def make(x, first, last):
        below = one[x] + inside * two[x] + three[x]
        for y in range(rows):
            held[y, x] = (sums[y, x] + below) * scale

    blocks(size, make, lambda i: copy(i).start())
    finish(copy, size)


def pass_kernel(place, total, one, two, out):
    def make(x, first, last):
        out[x] = jnp.where(place[0] == 2, total[x] + one[x], two[x])

    blocks(out.shape[0], make)


def shifts(axis):
    count = lax.axis_size(axis)
    up = [(i, i + 1) for i in range(count - 1)]
    return up, [(b, a) for a, b in up]


def program(tracer, crowding):
    rows, xs, zs, lanes = tracer.shape
    n = CHUNKS
    size = xs // n
    cells = rows * size * zs * lanes
    f32 = jnp.float32
    place = lax.axis_index("rows").astype(jnp.int32)
    tracer, place = lax.optimization_barrier((tracer, place))
    here = place.reshape(1)
    row_up, row_down = shifts("rows")
    col_up, col_down = shifts("cols")
    slab_up, slab_down = shifts("slabs")
    chunk_shape = pltpu.VMEM((rows, size, zs, lanes), f32)
    row_shape = pltpu.VMEM((size, zs, lanes), f32)
    edge_shape = pltpu.VMEM((rows, xs, 1, lanes), f32)
    side_shape = pltpu.VMEM((rows, 1, zs, lanes), f32)
    full = jax.ShapeDtypeStruct(tracer.shape, f32)
    scratch = [pltpu.VMEM((rows, size, zs, lanes), f32), pltpu.SemaphoreType.DMA((size // PLANES,))]

    def send_rows(lo, hi):
        return (lax.ppermute(hi, "rows", row_up), lax.ppermute(lo, "rows", row_down))

    def send_sides(low, high, zlow, zhigh):
        x = (lax.ppermute(high, "cols", col_up), lax.ppermute(low, "cols", col_down))
        z = (lax.ppermute(zhigh, "slabs", slab_up), lax.ppermute(zlow, "slabs", slab_down))
        return x, z

    def call(kernel, inputs, out_shape, per_cell, aliased=(), scratch=(), hbm_out=False):
        in_specs = [SMEM if array is here else VMEM for array in inputs] + [ANY if hbm_out else VMEM] * len(aliased)
        first = 0 if hbm_out else 3
        return pl.pallas_call(
            kernel,
            in_specs=in_specs,
            out_specs=[ANY if hbm_out and i == 0 else VMEM for i in range(len(out_shape))],
            out_shape=out_shape,
            input_output_aliases={len(inputs) + i: first + i for i in range(len(aliased))},
            scratch_shapes=list(scratch),
            compiler_params=pltpu.CompilerParams(vmem_limit_bytes=LIMIT),
            cost_estimate=pl.CostEstimate(flops=cells * per_cell, bytes_accessed=cells * 12, transcendentals=0),
        )(*inputs, *aliased)

    halo_y = []
    source = tracer
    for j in range(n):
        lo, hi = (source[r, j * size : (j + 1) * size] for r in (0, rows - 1))
        lo, hi, source = lax.optimization_barrier((lo, hi, source))
        halo_y.append(send_rows(lo, hi))
    halo_x, halo_z = send_sides(tracer[:, 0:1], tracer[:, xs - 1 : xs], tracer[:, :, 0:1], tracer[:, :, zs - 1 : zs])
    field = [tracer] * n
    whole = True

    def near(j):
        base = j * size if whole else 0
        low, xlo = (field[j - 1], (base if whole else size) - 1) if j else (halo_x[0], 0)
        high, xhi = (field[j + 1], base + size if whole else 0) if j < n - 1 else (halo_x[1], 0)
        return [field[j], crowding], [low, high, *halo_z], At(base, j * size, xlo, xhi)

    for _ in range(STEPS - 1):
        made, next_y, edges, z_edges = [], [], [], ()
        for j in range(n):
            first, sides, at = near(j)
            out, lo, hi, zlo, zhi, edge = call(
                functools.partial(step_kernel, at=at, edge_x=size - 1 if j == n - 1 else 0),
                [here, *first, *halo_y[j], *sides],
                [chunk_shape, row_shape, row_shape, edge_shape, edge_shape, side_shape],
                14,
                aliased=z_edges,
            )
            z_edges = (zlo, zhi)
            made.append(out)
            next_y.append(send_rows(lo, hi))
            edges.append(edge)
        halo_x, halo_z = send_sides(edges[0], edges[-1], *z_edges)
        field, halo_y, whole = made, next_y, False

    total = []
    for j in range(n):
        first, sides, at = near(j)
        total += call(functools.partial(total_kernel, at=at), [here, *first, *sides], [row_shape], 14)
    one, two, three = [None] * n, [None] * n, [None] * n
    one[0] = lax.ppermute(total[0], "rows", [(0, 1), (1, 2)])
    two[0] = lax.ppermute(total[0], "rows", [(0, 3)])
    two[1] = lax.ppermute(total[1], "rows", [(0, 3), (1, 0)])
    (passed,) = call(pass_kernel, [here, total[0], one[0], two[0]], [row_shape], 1)
    three[0] = lax.ppermute(passed, "rows", [(2, 3), (3, 2)])
    one[1] = lax.ppermute(total[1], "rows", row_up)
    three[1] = lax.ppermute(two[1], "rows", [(3, 2), (0, 3)])

    end, column = (), ()
    sums = []
    for j in range(n):
        first, sides, at = near(j)
        kernel = functools.partial(last_kernel, at=at)
        inputs = [here, *first, *halo_y[j], *sides]
        *end, partial = call(kernel, inputs, [full, chunk_shape], 18, end, scratch, True)
        sums.append(partial)
    for j in range(n):
        kernel = functools.partial(add_kernel, at=near(j)[2], scale=1.0 / (rows * lax.axis_size("rows")))
        column = call(kernel, [here, sums[j], one[j], two[j], three[j]], [full], 3, column, scratch, True)
    return column[0], end[0]


def solution(mesh):
    spec = P("rows", "cols", "slabs", None)
    return jax.shard_map(program, mesh=mesh, in_specs=(spec, spec), out_specs=(spec, spec), check_vma=False)
```
